32 devices in a mesh: seq: 16 (over z, y, core), tp: 2 (over x).
Axes of the slice: x: 2, y: 2, z: 4, core: 2. Of those that a mesh axis runs over, the one named last changes fastest.
Arguments:
- hidden: bfloat16 [2048, 7168], P('seq', 'tp'), may hold values from -6 to 6
- w_kv_down: bfloat16 [7168, 576], P('tp'), may hold values from -0.0625 to 0.0625
- kv_gain: float32 [512], replicated, may hold values from 0.1 to 1.9
- q_latent: bfloat16 [2048, 64, 512], P('seq', 'tp'), may hold values from -300 to 300
- q_rope: bfloat16 [2048, 4096], P('seq', 'tp'), may hold values from -6 to 6
- w_value: bfloat16 [64, 512, 128], P('tp'), may hold values from -0.75 to 0.75
Outputs:
- attended: bfloat16 [2048, 8192], P('seq', 'tp')
The draws below stay inside these ranges and needn't reach their ends.
All inputs are finite; a program needn't handle non-finite values.
Results may differ from the reference program's by a relative error of at most 0.0097.
Values may be sent and summed in bfloat16 or wider, within the bound.
No kernel may reach another device: no remote copies, remote signals or barrier semaphores. Data moves between devices by JAX's collectives and lax.ppermute only.
A program may use at most 128 MiB of HBM per device.

```python
import jax
import jax.numpy as jnp
from jax import lax

D = 7168
KV_RANK = 512
ROPE = 64
V_DIM = 128
HEADS = 64
TOKENS = 2048


def draw_q_latent(key, part):
    base = jnp.clip(jax.random.normal(key, (TOKENS, HEADS, KV_RANK), jnp.float32), -4.0, 4.0)
    return base.astype(jnp.bfloat16)


def block_levels(key, dims, split, least, high):
    def one(position, blocks):
        steps = jax.random.uniform(jax.random.fold_in(jax.random.fold_in(key, 6), position), (blocks,), jnp.float32, least / len(split), high / len(split))
        return jnp.repeat(jnp.exp(steps), dims[position] // blocks).reshape((-1,) + (1,) * (len(dims) - position - 1))

    level = one(*split[0])
    for cut in split[1:]:
        level = level * one(*cut)
    return level


def normal_values(key, extent, spread, reach, shards=(), kind=jnp.bfloat16):
    factor_of = block_levels(key, extent, shards, -0.22, 0.18) if shards else 1.0
    entries = jax.random.normal(key, extent, jnp.float32) * spread * factor_of
    return jnp.minimum(jnp.maximum(entries, -reach), reach).astype(kind)


def setup_inputs(seed: int = 0) -> dict:
    arg_keys = jax.random.split(jax.random.key(seed), 7)
    hidden = normal_values(arg_keys[0], (TOKENS, D), 1.0, 6.0, ((0, 16), (1, 2)))
    w_kv_down = normal_values(arg_keys[1], (D, KV_RANK + ROPE), D ** -0.5, 0.0625, ((0, 2),))
    kv_gain = jnp.clip(1.0 + 0.18 * jax.random.normal(arg_keys[2], (KV_RANK,), jnp.float32), 0.1, 1.9)
    q_latent = draw_q_latent(jax.random.fold_in(arg_keys[6], 71), 0)
    q_rope = normal_values(arg_keys[4], (TOKENS, HEADS * ROPE), 1.0, 6.0, ((0, 16), (1, 2)))
    w_value = normal_values(arg_keys[5], (HEADS, KV_RANK, V_DIM), (KV_RANK // 8) ** -0.5, 0.75, ((0, 2),))
    return {"hidden": hidden, "w_kv_down": w_kv_down, "kv_gain": kv_gain, "q_latent": q_latent, "q_rope": q_rope, "w_value": w_value}


SCORE_SCALE = 192.0 ** (-0.5)
ROPE_BASE = 10000.0
EPSILON = 1e-06

def rotate(values, positions):
    full_width = values.shape[-1]
    half_width = full_width // 2
    frequency = ROPE_BASE ** (-jnp.arange(half_width, dtype=jnp.float32) * 2.0 / full_width)
    angles = positions.astype(jnp.float32)[:, None] * frequency[None, :]
    angle_shape = (angles.shape[0],) + (1,) * (values.ndim - 2) + (half_width,)
    cosine = jnp.cos(angles).reshape(angle_shape)
    sine_part = jnp.sin(angles).reshape(angle_shape)
    first_half = values[..., :half_width]
    second_half = values[..., half_width:]
    return jnp.concatenate([first_half * cosine - second_half * sine_part, first_half * sine_part + second_half * cosine], -1)

def finish(projection, kv_gain, positions):
    latent_part = projection[:, :KV_RANK]
    mean_square = lax.optimization_barrier(jnp.mean(latent_part * latent_part, axis=-1, keepdims=True))
    normed = latent_part * lax.rsqrt(mean_square + EPSILON) * kv_gain[None, :]
    rope_part = rotate(projection[:, KV_RANK:], positions)
    return jnp.concatenate([normed, rope_part], -1).astype(jnp.bfloat16)

def reference(hidden, w_kv_down, kv_gain, q_latent, q_rope, w_value):
    positions = jnp.arange(TOKENS, dtype=jnp.int32)
    projection = jnp.dot(hidden, w_kv_down, preferred_element_type=jnp.float32)
    key_rows = lax.optimization_barrier(finish(projection, kv_gain, positions))
    key_float = key_rows.astype(jnp.float32)
    rope_query = rotate(q_rope.astype(jnp.float32).reshape(TOKENS, HEADS, ROPE), positions).astype(jnp.bfloat16)
    rope_query = lax.optimization_barrier(rope_query)
    queries = jnp.concatenate([q_latent, rope_query], -1)
    block_rows = min(256, TOKENS)
    block_count = TOKENS // block_rows

    def attend_block(block_index):
        first_row = block_index * block_rows
        query_rows = lax.dynamic_slice_in_dim(queries, first_row, block_rows, 0).astype(jnp.float32)
        scores = jnp.einsum('qhc,kc->hqk', query_rows, key_float) * SCORE_SCALE
        query_positions = first_row + jnp.arange(block_rows, dtype=jnp.int32)
        allowed = (positions[None, :] <= query_positions[:, None])[None]
        scores = jnp.where(allowed, scores, -1e+30)
        row_max = lax.optimization_barrier(jnp.max(scores, axis=-1, keepdims=True))
        weights = jnp.where(allowed, jnp.exp(scores - row_max), 0.0)
        weight_total = lax.optimization_barrier(jnp.sum(weights, axis=-1))
        rounded = lax.optimization_barrier(weights.astype(jnp.bfloat16))
        mixed_keys = jnp.einsum('hqk,kc->hqc', rounded.astype(jnp.float32), key_float[:, :KV_RANK])
        latent_out = lax.optimization_barrier((mixed_keys / weight_total[..., None]).astype(jnp.bfloat16))
        projected = jnp.einsum('hqc,hcv->qhv', latent_out.astype(jnp.float32), w_value.astype(jnp.float32))
        return projected.astype(jnp.bfloat16).reshape(block_rows, HEADS * V_DIM)
    results = lax.map(attend_block, jnp.arange(block_count, dtype=jnp.int32))
    return results.reshape(TOKENS, HEADS * V_DIM)
```

```python
import functools

import jax
import jax.numpy as jnp
from jax import lax
from jax.experimental import pallas as pl
from jax.experimental.pallas import tpu as pltpu
from jax.sharding import PartitionSpec as P

KV_RANK = 512
ROPE = 64
LANES = 128
GROUP = 4

SCORE_SCALE = 192.0 ** (-0.5)
LOG2_E = 1.4426950408889634
EXP2_SCALE = SCORE_SCALE * LOG2_E
ROPE_BASE = 10000.0
EPSILON = 1e-06
MASKED = -1e30
VMEM_LIMIT = 56 * 1024 * 1024


def tables(positions):
    half = ROPE // 2
    frequency = ROPE_BASE ** (-jnp.arange(half, dtype=jnp.float32) * 2.0 / ROPE)
    angles = positions.astype(jnp.float32)[:, None] * frequency[None, :]
    cosine, sine = jnp.cos(angles), jnp.sin(angles)
    return jnp.concatenate([cosine, cosine], -1), jnp.concatenate([-sine, sine], -1)


def swap_halves(values):
    half = ROPE // 2
    return jnp.concatenate([values[..., half:], values[..., :half]], -1)


def project_kernel(hidden_ref, weight_ref, out_ref):
    part = lax.dot_general(
        hidden_ref[...],
        weight_ref[...],
        (((1,), (1,)), ((), ())),
        preferred_element_type=jnp.float32,
    )

    @pl.when(pl.program_id(0) == 0)
    def _():
        out_ref[...] = part

    @pl.when(pl.program_id(0) > 0)
    def _():
        out_ref[...] += part


def down_project(hidden, weight_t):
    rows, depth = hidden.shape
    width = weight_t.shape[0]
    step = next(s for s in (1792, 896, 512, 256, 128) if depth % s == 0)
    return pl.pallas_call(
        project_kernel,
        out_shape=jax.ShapeDtypeStruct((rows, width), jnp.float32),
        grid=(depth // step,),
        in_specs=[
            pl.BlockSpec((rows, step), lambda k: (0, k)),
            pl.BlockSpec((width, step), lambda k: (0, k)),
        ],
        out_specs=pl.BlockSpec((rows, width), lambda k: (0, 0)),
        cost_estimate=pl.CostEstimate(
            flops=2 * rows * depth * width, bytes_accessed=2 * depth * (rows + width), transcendentals=0
        ),
        name="down_project",
    )(hidden, weight_t)


def finish_kernel(own_ref, other_ref, gain_ref, cos_ref, sin_ref, out_ref):
    projection = own_ref[...] + other_ref[...]
    latent = projection[:, :KV_RANK]
    mean_square = jnp.mean(latent * latent, axis=-1, keepdims=True)
    normed = latent * lax.rsqrt(mean_square + EPSILON) * gain_ref[...]
    rope = projection[:, KV_RANK:]
    rotated = rope * cos_ref[...] + swap_halves(rope) * sin_ref[...]
    out_ref[:, :KV_RANK] = normed.astype(jnp.bfloat16)
    out_ref[:, KV_RANK:] = rotated.astype(jnp.bfloat16)


def finish(own, other, gain, cosine, sine):
    return pl.pallas_call(
        finish_kernel,
        out_shape=jax.ShapeDtypeStruct(own.shape, jnp.bfloat16),
        name="finish_keys",
    )(own, other, gain[None, :], cosine, sine)


def attend_kernel(chunks, latent_ref, rope_ref, bias_ref, row_bias_ref, *refs):
    *key_refs, value_ref, out_ref = refs
    heads, tokens = latent_ref.shape[:2]
    rows = heads * tokens
    query = jnp.concatenate(
        [latent_ref[...].reshape(rows, KV_RANK), rope_ref[...].reshape(rows, ROPE)], -1
    )
    top = total = mixed = None
    column = 0
    for chunk in chunks:
        parts = [key_refs[i][begin : begin + size, :] for i, begin, size in chunk]
        keys = parts[0] if len(parts) == 1 else jnp.concatenate(parts, 0)
        count = keys.shape[0]
        scores = lax.dot_general(
            query, keys, (((1,), (1,)), ((), ())), preferred_element_type=jnp.float32
        )
        if top is None:
            scores = (scores.reshape(heads, tokens, count) + bias_ref[...][None]).reshape(rows, count)
        else:
            scores = scores + row_bias_ref[:1, column : column + count]
            column += count
        chunk_top = jnp.max(scores, axis=-1, keepdims=True)
        new_top = chunk_top if top is None else jnp.maximum(top, chunk_top)
        weights = jnp.exp2((scores - new_top) * EXP2_SCALE)
        chunk_total = jnp.sum(weights, axis=-1, keepdims=True)
        chunk_mixed = jnp.dot(
            weights.astype(jnp.bfloat16), keys[:, :KV_RANK], preferred_element_type=jnp.float32
        )
        if top is None:
            total, mixed = chunk_total, chunk_mixed
        else:
            rescale = jnp.exp2((top - new_top) * EXP2_SCALE)
            total = total * rescale + chunk_total
            mixed = mixed * rescale + chunk_mixed
        top = new_top
    latent_out = (mixed / total).astype(jnp.bfloat16)
    width = value_ref.shape[2]
    for h in range(heads):
        out_ref[:, h * width : (h + 1) * width] = jnp.dot(
            latent_out[h * tokens : (h + 1) * tokens],
            value_ref[h],
            preferred_element_type=jnp.float32,
        ).astype(jnp.bfloat16)


def plane_first(keys, tokens):
    columns = []
    for i, key in enumerate(keys):
        length = key.shape[0] * len(keys) // GROUP
        columns += [(i, begin, length) for begin in range(0, key.shape[0], length)]
    chunks = [[(i, begin, tokens) for i, begin, _ in columns]]
    pieces = [
        (i, begin + tokens * d, tokens)
        for i, begin, length in columns
        for d in range(1, length // tokens)
    ]
    chunks += [pieces[p : p + GROUP] for p in range(0, len(pieces), GROUP)]
    return chunks


def attend(latent, rope, bias, row_bias, keys, w_value):
    all_heads, tokens, _ = latent.shape
    heads = next(h for h in (8, 4, 2, 1) if all_heads % h == 0)
    chunks = plane_first(keys, tokens)
    count = sum(k.shape[0] for k in keys)
    width = w_value.shape[2]
    by_head = lambda a: pl.BlockSpec((heads,) + a.shape[1:], lambda g: (g, 0, 0))
    whole = lambda a: pl.BlockSpec(a.shape, lambda g: (0,) * a.ndim)
    return pl.pallas_call(
        functools.partial(attend_kernel, chunks),
        out_shape=jax.ShapeDtypeStruct((tokens, all_heads * width), jnp.bfloat16),
        grid=(all_heads // heads,),
        in_specs=[by_head(latent), by_head(rope), whole(bias), whole(row_bias)]
        + [whole(k) for k in keys]
        + [by_head(w_value)],
        out_specs=pl.BlockSpec((tokens, heads * width), lambda g: (0, g)),
        compiler_params=pltpu.CompilerParams(vmem_limit_bytes=VMEM_LIMIT),
        cost_estimate=pl.CostEstimate(
            flops=2 * all_heads * tokens * count * (2 * KV_RANK + ROPE),
            bytes_accessed=2 * all_heads * tokens * (KV_RANK + ROPE),
            transcendentals=all_heads * tokens * count,
        ),
        name="attend",
    )(latent, rope, bias, row_bias, *keys, w_value)


def shards(seq_size, tp_size, hidden, w_kv_down, kv_gain, q_latent, q_rope, w_value):
    tokens = hidden.shape[0]
    heads = q_latent.shape[1]
    index = lax.axis_index("seq")
    positions = index * tokens + jnp.arange(tokens, dtype=jnp.int32)

    def from_seq(value, xor):
        return lax.ppermute(value, "seq", [(i, i ^ xor) for i in range(seq_size)])

    def from_below(value, planes):
        shift = planes * GROUP
        return lax.ppermute(value, "seq", [(i, i + shift) for i in range(seq_size - shift)])

    own = down_project(hidden, w_kv_down.T)
    stride = 1
    while True:
        other = lax.ppermute(own, "tp", [(i, i ^ stride) for i in range(tp_size)])
        stride *= 2
        if stride >= tp_size:
            break
        own = own + other
    cosine, sine = tables(positions)
    key_here = finish(own, other, kv_gain, cosine, sine)

    latent = jnp.transpose(q_latent, (1, 0, 2))
    rope = q_rope.astype(jnp.float32).reshape(tokens, heads, ROPE)
    rope = rope * cosine[:, None, :] + swap_halves(rope) * sine[:, None, :]
    rope = jnp.transpose(rope.astype(jnp.bfloat16), (1, 0, 2))

    planes = seq_size // GROUP
    below = [from_below(key_here, d) for d in range(1, planes)]
    column = jnp.concatenate([key_here] + below, 0)
    column_y = from_seq(column, 2)
    pair = jnp.concatenate([column, column_y], 0)
    pair_core = from_seq(pair, 1)

    start = lambda xor: (index ^ xor) * tokens + jnp.arange(tokens, dtype=jnp.int32)
    key_positions = jnp.concatenate([start(0), start(2), start(1), start(3)])
    bias = jnp.where(key_positions[None, :] <= positions[:, None], 0.0, MASKED)
    bias = bias.astype(jnp.float32)
    levels = jnp.repeat(jnp.arange(planes)[1:], tokens)
    row_bias = jnp.where(index // GROUP >= levels, 0.0, MASKED).astype(jnp.float32)
    row_bias = jnp.broadcast_to(jnp.tile(row_bias, GROUP)[None], (8, GROUP * levels.shape[0]))
    return attend(latent, rope, bias, row_bias, [pair, pair_core], w_value)


def solution(mesh):
    placed = (
        P("seq", "tp"),
        P("tp", None),
        P(),
        P("seq", "tp", None),
        P("seq", "tp"),
        P("tp", None, None),
    )
    body = functools.partial(shards, mesh.shape["seq"], mesh.shape["tp"])
    return jax.shard_map(
        body, mesh=mesh, in_specs=placed, out_specs=P("seq", "tp"), check_vma=False
    )
```

```python
import functools

import jax
import jax.numpy as jnp
from jax import lax
from jax.experimental import pallas as pl
from jax.experimental.pallas import tpu as pltpu
from jax.sharding import PartitionSpec as P


KV_RANK = 512
ROPE = 64
LANES = 128
GROUP = 4

SCORE_SCALE = 192.0 ** (-0.5)
LOG2_E = 1.4426950408889634
EXP2_SCALE = SCORE_SCALE * LOG2_E
ROPE_BASE = 10000.0
EPSILON = 1e-06
MASKED = -1e30
CHUNK = 4
VMEM_LIMIT = 24 * 1024 * 1024
SMALL_VMEM = 8 * 1024 * 1024
FULL_VMEM = 60 * 1024 * 1024
PROJECT_STEPS = (896, 512, 256, 128)


def tables(positions):
    half = ROPE // 2
    frequency = ROPE_BASE ** (-jnp.arange(half, dtype=jnp.float32) * 2.0 / ROPE)
    angles = positions.astype(jnp.float32)[:, None] * frequency[None, :]
    cosine, sine = jnp.cos(angles), jnp.sin(angles)
    return jnp.concatenate([cosine, cosine], -1), jnp.concatenate([-sine, sine], -1)


def swap_halves(values):
    half = ROPE // 2
    return jnp.concatenate([values[..., half:], values[..., :half]], -1)


def project_kernel(hidden_ref, weight_ref, out_ref, hidden_vmem, weight_vmem, sems):
    depth = hidden_ref.shape[1]
    steps = sems.shape[1]
    size = depth // steps
    copies = []
    for k in range(steps):
        at = pl.ds(k * size, size)
        pair = (
            pltpu.make_async_copy(weight_ref.at[:, at], weight_vmem.at[:, at], sems.at[0, k]),
            pltpu.make_async_copy(hidden_ref.at[:, at], hidden_vmem.at[:, at], sems.at[1, k]),
        )
        for copy in pair:
            copy.start()
        copies.append(pair)
    total = None
    for k, pair in enumerate(copies):
        for copy in pair:
            copy.wait()
        at = slice(k * size, (k + 1) * size)
        part = lax.dot_general(
            hidden_vmem[:, at],
            weight_vmem[:, at],
            (((1,), (1,)), ((), ())),
            preferred_element_type=jnp.float32,
        )
        total = part if total is None else total + part
    out_ref[...] = total


def down_project(hidden, weight_t):
    rows, depth = hidden.shape
    width = weight_t.shape[0]
    size = next(s for s in PROJECT_STEPS if depth % s == 0)
    return pl.pallas_call(
        project_kernel,
        out_shape=jax.ShapeDtypeStruct((rows, width), jnp.float32),
        in_specs=[pl.BlockSpec(memory_space=pltpu.HBM)] * 2,
        out_specs=pl.BlockSpec(memory_space=pltpu.VMEM),
        scratch_shapes=[
            pltpu.VMEM(hidden.shape, hidden.dtype),
            pltpu.VMEM(weight_t.shape, weight_t.dtype),
            pltpu.SemaphoreType.DMA((2, depth // size)),
        ],
        cost_estimate=pl.CostEstimate(
            flops=2 * rows * depth * width, bytes_accessed=2 * depth * (rows + width), transcendentals=0
        ),
        compiler_params=pltpu.CompilerParams(vmem_limit_bytes=FULL_VMEM),
        name="down_project",
    )(hidden, weight_t)


def finish_kernel(own_ref, other_ref, gain_ref, cos_ref, sin_ref, ready_ref, out_ref):
    del ready_ref
    projection = own_ref[...] + other_ref[...]
    latent = projection[:, :KV_RANK]
    mean_square = jnp.mean(latent * latent, axis=-1, keepdims=True)
    normed = latent * lax.rsqrt(mean_square + EPSILON) * gain_ref[...]
    rope = projection[:, KV_RANK:]
    rotated = rope * cos_ref[...] + swap_halves(rope) * sin_ref[...]
    out_ref[:, :KV_RANK] = normed.astype(jnp.bfloat16)
    out_ref[:, KV_RANK:] = rotated.astype(jnp.bfloat16)


def finish(own, other, gain, cosine, sine, ready):
    return pl.pallas_call(
        finish_kernel,
        out_shape=jax.ShapeDtypeStruct(own.shape, jnp.bfloat16),
        in_specs=[pl.BlockSpec(memory_space=pltpu.VMEM)] * 5 + [pl.BlockSpec(memory_space=pl.ANY)],
        out_specs=pl.BlockSpec(memory_space=pltpu.VMEM),
        compiler_params=pltpu.CompilerParams(vmem_limit_bytes=SMALL_VMEM),
        name="finish_keys",
    )(own, other, gain[None, :], cosine, sine, ready)


def block_bias(index, tag, tokens, rows):
    kind, amount = tag
    if kind == "plane":
        key = (index ^ amount) * tokens + lax.broadcasted_iota(jnp.int32, (rows, tokens), 1)
        query = index * tokens + lax.broadcasted_iota(jnp.int32, (rows, tokens), 0)
        return jnp.where(key <= query, 0.0, MASKED)
    return jnp.full((rows, tokens), jnp.where(index // GROUP >= amount, 0.0, MASKED), jnp.float32)


def attend_kernel(tags, first, last, index_ref, latent_ref, rope_ref, *refs):
    key_refs, rest = refs[: len(tags)], list(refs[len(tags) :])
    heads, tokens = latent_ref.shape[:2]
    rows = heads * tokens
    index = index_ref[0]
    query = jnp.concatenate(
        [latent_ref[...].reshape(rows, KV_RANK), rope_ref[...].reshape(rows, ROPE)], -1
    )
    wide = lambda column: jnp.broadcast_to(column, (rows, LANES))
    spread = lambda value, width: jnp.concatenate([value] * (width // LANES), -1)
    top = total = mixed = None
    if not first:
        mixed, top, total = (ref[...].reshape(rows, ref.shape[2]) for ref in rest[:3])
        rest = rest[3:]
    for begin in range(0, len(tags), CHUNK):
        group = range(begin, min(begin + CHUNK, len(tags)))
        keys = jnp.concatenate([key_refs[i][...] for i in group], 0)
        count = keys.shape[0]
        scores = lax.dot_general(
            query, keys, (((1,), (1,)), ((), ())), preferred_element_type=jnp.float32
        )
        plane = tags[begin][0] == "plane"
        bias = jnp.concatenate(
            [block_bias(index, tags[i], tokens, tokens if plane else 1) for i in group], -1
        )
        if plane:
            scores = (scores.reshape(heads, tokens, count) + bias[None]).reshape(rows, count)
        else:
            scores = scores + bias
        chunk_top = wide(jnp.max(scores, axis=-1, keepdims=True))
        new_top = chunk_top if top is None else jnp.maximum(top, chunk_top)
        weights = jnp.exp2((scores - spread(new_top, count)) * EXP2_SCALE)
        chunk_total = wide(jnp.sum(weights, axis=-1, keepdims=True))
        chunk_mixed = jnp.dot(
            weights.astype(jnp.bfloat16), keys[:, :KV_RANK], preferred_element_type=jnp.float32
        )
        if top is None:
            total, mixed = chunk_total, chunk_mixed
        else:
            rescale = jnp.exp2((top - new_top) * EXP2_SCALE)
            total = total * rescale + chunk_total
            mixed = mixed * spread(rescale, KV_RANK) + chunk_mixed
        top = new_top
    if last:
        value_ref, out_ref = rest
        latent_out = (mixed / spread(total, KV_RANK)).astype(jnp.bfloat16)
        width = value_ref.shape[2]
        for h in range(heads):
            out_ref[:, h * width : (h + 1) * width] = jnp.dot(
                latent_out[h * tokens : (h + 1) * tokens],
                value_ref[h],
                preferred_element_type=jnp.float32,
            ).astype(jnp.bfloat16)
    else:
        for ref, value in zip(rest, (mixed, top, total)):
            ref[...] = value.reshape(ref.shape)


def attend(index, latent, rope, tagged, state=(), w_value=None):
    first, last = not state, w_value is not None
    tags, keys = zip(*tagged)
    all_heads, tokens, _ = latent.shape
    heads = next(h for h in (8, 4, 2, 1) if all_heads % h == 0)
    count = sum(k.shape[0] for k in keys)
    by_head = lambda a: pl.BlockSpec((heads,) + a.shape[1:], lambda g: (g, 0, 0))
    whole = lambda a: pl.BlockSpec(a.shape, lambda g: (0,) * a.ndim)
    operands = [index, latent, rope, *keys, *state]
    in_specs = [pl.BlockSpec(memory_space=pltpu.SMEM), by_head(latent), by_head(rope)]
    in_specs += [whole(k) for k in keys] + [by_head(a) for a in state]
    if last:
        width = w_value.shape[2]
        operands.append(w_value)
        in_specs.append(by_head(w_value))
        out_shape = jax.ShapeDtypeStruct((tokens, all_heads * width), jnp.bfloat16)
        out_specs = pl.BlockSpec((tokens, heads * width), lambda g: (0, g))
    else:
        out_shape = tuple(
            jax.ShapeDtypeStruct((all_heads, tokens, width), jnp.float32)
            for width in (KV_RANK, LANES, LANES)
        )
        out_specs = tuple(by_head(a) for a in out_shape)
    return pl.pallas_call(
        functools.partial(attend_kernel, tags, first, last),
        out_shape=out_shape,
        grid=(all_heads // heads,),
        in_specs=in_specs,
        out_specs=out_specs,
        input_output_aliases={} if first or last else {len(operands) - len(state) + i: i for i in range(len(state))},
        compiler_params=pltpu.CompilerParams(vmem_limit_bytes=VMEM_LIMIT),
        cost_estimate=pl.CostEstimate(
            flops=2 * all_heads * tokens * count * (2 * KV_RANK + ROPE),
            bytes_accessed=2 * all_heads * tokens * (KV_RANK + ROPE),
            transcendentals=all_heads * tokens * count,
        ),
        name="attend",
    )(*operands)


def shards(seq_size, tp_size, hidden, w_kv_down, kv_gain, q_latent, q_rope, w_value):
    tokens = hidden.shape[0]
    heads = q_latent.shape[1]
    index = lax.axis_index("seq")
    positions = index * tokens + jnp.arange(tokens, dtype=jnp.int32)
    index = index.reshape(1)

    def from_seq(value, xor):
        return lax.ppermute(value, "seq", [(i, i ^ xor) for i in range(seq_size)])

    def from_below(value, planes):
        shift = planes * GROUP
        return lax.ppermute(value, "seq", [(i, i + shift) for i in range(seq_size - shift)])

    own = down_project(hidden, w_kv_down.T)
    stride = 1
    while True:
        other = lax.ppermute(own, "tp", [(i, i ^ stride) for i in range(tp_size)])
        stride *= 2
        if stride >= tp_size:
            break
        own = own + other
    cosine, sine = tables(positions)
    latent = jnp.transpose(q_latent, (1, 0, 2))
    key_here = finish(own, other, kv_gain, cosine, sine, latent)

    rope = q_rope.astype(jnp.float32).reshape(tokens, heads, ROPE)
    rope = rope * cosine[:, None, :] + swap_halves(rope) * sine[:, None, :]
    rope = jnp.transpose(rope.astype(jnp.bfloat16), (1, 0, 2))

    levels = range(1, seq_size // GROUP)
    key_y = from_seq(key_here, 2)
    below = {d: from_below(key_here, d) for d in levels}
    plane = [key_here, key_y, from_seq(key_here, 1), from_seq(key_y, 1)]
    below_y = {d: from_seq(below[d], 2) for d in levels}
    below_core = {d: from_seq(below[d], 1) for d in levels}
    below_yc = {d: from_seq(below_y[d], 1) for d in levels}
    tag = lambda group: [(("below", d), group[d]) for d in group]

    state = attend(index, latent, rope, [(("plane", x), k) for x, k in zip((0, 2, 1, 3), plane)])
    early = tag(below) + tag({1: below_y[1]})
    late = tag({d: below_y[d] for d in levels if d > 1}) + tag(below_core) + tag(below_yc)
    state = attend(index, latent, rope, early, state=state)
    return attend(index, latent, rope, late, state=state, w_value=w_value)


def solution(mesh):
    placed = (
        P("seq", "tp"),
        P("tp", None),
        P(),
        P("seq", "tp", None),
        P("seq", "tp"),
        P("tp", None, None),
    )
    body = functools.partial(shards, mesh.shape["seq"], mesh.shape["tp"])

    return jax.shard_map(
        body, mesh=mesh, in_specs=placed, out_specs=P("seq", "tp"), check_vma=False
    )
```

```python
import functools

import jax
import jax.numpy as jnp
from jax import lax
from jax.experimental import pallas as pl
from jax.experimental.pallas import tpu as pltpu
from jax.sharding import PartitionSpec as P


KV_RANK = 512
ROPE = 64
LANES = 128
GROUP = 4

SCORE_SCALE = 192.0 ** (-0.5)
LOG2_E = 1.4426950408889634
EXP2_SCALE = SCORE_SCALE * LOG2_E
ROPE_BASE = 10000.0
EPSILON = 1e-06
MASKED = -1e30
CHUNK = 4
VMEM_LIMIT = 24 * 1024 * 1024
SMALL_VMEM = 8 * 1024 * 1024
FULL_VMEM = 60 * 1024 * 1024
PROJECT_STEPS = (896, 512, 256, 128)


def tables(positions):
    half = ROPE // 2
    frequency = ROPE_BASE ** (-jnp.arange(half, dtype=jnp.float32) * 2.0 / ROPE)
    angles = frequency[:, None] * positions.astype(jnp.float32)[None, :]
    return jnp.cos(angles), jnp.sin(angles)


def query_tables(positions):
    half = ROPE // 2
    frequency = ROPE_BASE ** (-jnp.arange(half, dtype=jnp.float32) * 2.0 / ROPE)
    angles = positions.astype(jnp.float32)[:, None] * frequency[None, :]
    cosine, sine = jnp.cos(angles), jnp.sin(angles)
    return jnp.concatenate([cosine] * 4, -1), jnp.concatenate([-sine, sine] * 2, -1)


def project_kernel(hidden_ref, weight_ref, out_ref, hidden_vmem, weight_vmem, sems):
    depth = hidden_ref.shape[1]
    steps = sems.shape[1]
    size = depth // steps
    copies = []
    for k in range(steps):
        at = pl.ds(k * size, size)
        pair = (
            pltpu.make_async_copy(weight_ref.at[:, at], weight_vmem.at[:, at], sems.at[0, k]),
            pltpu.make_async_copy(hidden_ref.at[:, at], hidden_vmem.at[:, at], sems.at[1, k]),
        )
        for copy in pair:
            copy.start()
        copies.append(pair)
    total = None
    for k, pair in enumerate(copies):
        for copy in pair:
            copy.wait()
        at = slice(k * size, (k + 1) * size)
        part = lax.dot_general(
            weight_vmem[:, at],
            hidden_vmem[:, at],
            (((1,), (1,)), ((), ())),
            preferred_element_type=jnp.float32,
        )
        total = part if total is None else total + part
    out_ref[...] = total


def down_project(hidden, weight_t):
    rows, depth = hidden.shape
    width = weight_t.shape[0]
    size = next(s for s in PROJECT_STEPS if depth % s == 0)
    return pl.pallas_call(
        project_kernel,
        out_shape=jax.ShapeDtypeStruct((width, rows), jnp.float32),
        in_specs=[pl.BlockSpec(memory_space=pltpu.HBM)] * 2,
        out_specs=pl.BlockSpec(memory_space=pltpu.VMEM),
        scratch_shapes=[
            pltpu.VMEM(hidden.shape, hidden.dtype),
            pltpu.VMEM(weight_t.shape, weight_t.dtype),
            pltpu.SemaphoreType.DMA((2, depth // size)),
        ],
        cost_estimate=pl.CostEstimate(
            flops=2 * rows * depth * width, bytes_accessed=2 * depth * (rows + width), transcendentals=0
        ),
        compiler_params=pltpu.CompilerParams(vmem_limit_bytes=FULL_VMEM),
        name="down_project",
    )(hidden, weight_t)


def finish_kernel(own_ref, other_ref, gain_ref, cos_ref, sin_ref, latent_ref, rope_ref, out_ref):
    del latent_ref, rope_ref
    projection = own_ref[...] + other_ref[...]
    latent = projection[:KV_RANK]
    mean_square = jnp.mean(latent * latent, axis=0, keepdims=True)
    normed = latent * lax.rsqrt(mean_square + EPSILON) * gain_ref[...]
    half = ROPE // 2
    first, second = projection[KV_RANK : KV_RANK + half], projection[KV_RANK + half :]
    cosine, sine = cos_ref[...], sin_ref[...]
    keys = [normed, first * cosine - second * sine, first * sine + second * cosine]
    out_ref[...] = jnp.concatenate(keys, 0).astype(jnp.bfloat16)


def finish(own, other, gain, cosine, sine, latent, rope):
    return pl.pallas_call(
        finish_kernel,
        out_shape=jax.ShapeDtypeStruct(own.shape, jnp.bfloat16),
        in_specs=[pl.BlockSpec(memory_space=pltpu.VMEM)] * 5 + [pl.BlockSpec(memory_space=pl.ANY)] * 2,
        out_specs=pl.BlockSpec(memory_space=pltpu.VMEM),
        compiler_params=pltpu.CompilerParams(vmem_limit_bytes=SMALL_VMEM),
        name="finish_keys",
    )(own, other, gain, cosine, sine, latent, rope)


def rotate_kernel(query_ref, cos_ref, sin_ref, out_ref):
    cosine, sine = cos_ref[...], sin_ref[...]
    half = ROPE // 2
    lower = lax.broadcasted_iota(jnp.int32, cosine.shape, 1) % ROPE < half
    for pair in range(query_ref.shape[1] // (2 * ROPE)):
        value = query_ref[:, pair * 2 * ROPE : (pair + 1) * 2 * ROPE].astype(jnp.float32)
        up, down = pltpu.roll(value, 2 * ROPE - half, 1), pltpu.roll(value, half, 1)
        rotated = value * cosine + jnp.where(lower, up, down) * sine
        out_ref[2 * pair] = rotated[:, :ROPE].astype(jnp.bfloat16)
        out_ref[2 * pair + 1] = rotated[:, ROPE:].astype(jnp.bfloat16)


def rotate(query, cosine, sine, heads):
    return pl.pallas_call(
        rotate_kernel,
        out_shape=jax.ShapeDtypeStruct((heads, query.shape[0], ROPE), jnp.bfloat16),
        compiler_params=pltpu.CompilerParams(vmem_limit_bytes=SMALL_VMEM),
        name="rotate_queries",
    )(query, cosine, sine)


def block_bias(index, tag, tokens, rows):
    kind, amount = tag
    if kind == "plane":
        key = (index ^ amount) * tokens + lax.broadcasted_iota(jnp.int32, (rows, tokens), 1)
        query = index * tokens + lax.broadcasted_iota(jnp.int32, (rows, tokens), 0)
        return jnp.where(key <= query, 0.0, MASKED)
    return jnp.full((rows, tokens), jnp.where(index // GROUP >= amount, 0.0, MASKED), jnp.float32)


def attend_kernel(tags, first, last, index_ref, latent_ref, rope_ref, *refs):
    key_refs, rest = refs[: len(tags)], list(refs[len(tags) :])
    heads, tokens = latent_ref.shape[:2]
    rows = heads * tokens
    index = index_ref[0]
    state_refs = [] if first else rest[:3]
    rest = rest[len(state_refs) :]
    groups = [range(b, min(b + CHUNK, len(tags))) for b in range(0, len(tags), CHUNK)]
    wide = lambda column: jnp.broadcast_to(column, (rows, LANES))
    spread = lambda value, width: jnp.concatenate([value] * (width // LANES), -1)

    def run(groups):
        top = total = mixed = None
        if not first:
            mixed, top, total = (ref[...].reshape(rows, ref.shape[2]) for ref in state_refs)
        if groups:
            query = jnp.concatenate(
                [latent_ref[...].reshape(rows, KV_RANK), rope_ref[...].reshape(rows, ROPE)], -1
            )
        for group in groups:
            keys = jnp.concatenate([key_refs[i][...] for i in group], 1)
            count = keys.shape[1]
            scores = jnp.dot(query, keys, preferred_element_type=jnp.float32)
            plane = tags[group[0]][0] == "plane"
            bias = jnp.concatenate(
                [block_bias(index, tags[i], tokens, tokens if plane else 1) for i in group], -1
            )
            if plane:
                scores = (scores.reshape(heads, tokens, count) + bias[None]).reshape(rows, count)
            else:
                scores = scores + bias
            chunk_top = wide(jnp.max(scores, axis=-1, keepdims=True))
            new_top = chunk_top if top is None else jnp.maximum(top, chunk_top)
            weights = jnp.exp2((scores - spread(new_top, count)) * EXP2_SCALE)
            chunk_total = wide(jnp.sum(weights, axis=-1, keepdims=True))
            chunk_mixed = lax.dot_general(
                weights.astype(jnp.bfloat16),
                keys[:KV_RANK],
                (((1,), (1,)), ((), ())),
                preferred_element_type=jnp.float32,
            )
            if top is None:
                total, mixed = chunk_total, chunk_mixed
            else:
                rescale = jnp.exp2((top - new_top) * EXP2_SCALE)
                total = total * rescale + chunk_total
                mixed = mixed * spread(rescale, KV_RANK) + chunk_mixed
            top = new_top
        if last:
            value_ref, out_ref = rest
            latent_out = (mixed / spread(total, KV_RANK)).astype(jnp.bfloat16)
            width = value_ref.shape[2]
            for h in range(heads):
                out_ref[:, h * width : (h + 1) * width] = jnp.dot(
                    latent_out[h * tokens : (h + 1) * tokens],
                    value_ref[h],
                    preferred_element_type=jnp.float32,
                ).astype(jnp.bfloat16)
        else:
            for ref, value in zip(rest, (mixed, top, total)):
                ref[...] = value.reshape(ref.shape)

    if first:
        run(groups)
        return
    lowest = [min(tags[i][1] for i in group) for group in groups]
    needed = sum((index // GROUP >= level).astype(jnp.int32) for level in lowest)
    cases = sorted({0, 1, len(groups)})
    for below, case in zip([-1] + cases, cases):

        @pl.when((needed > below) & (needed <= case))
        def _():
            run(groups[:case])


def attend(index, latent, rope, tagged, state=(), w_value=None):
    first, last = not state, w_value is not None
    tags, keys = zip(*tagged)
    all_heads, tokens, _ = latent.shape
    heads = next(h for h in (8, 4, 2, 1) if all_heads % h == 0)
    count = sum(k.shape[1] for k in keys)
    by_head = lambda a: pl.BlockSpec((heads,) + a.shape[1:], lambda g: (g, 0, 0))
    whole = lambda a: pl.BlockSpec(a.shape, lambda g: (0,) * a.ndim)
    operands = [index, latent, rope, *keys, *state]
    in_specs = [pl.BlockSpec(memory_space=pltpu.SMEM), by_head(latent), by_head(rope)]
    in_specs += [whole(k) for k in keys] + [by_head(a) for a in state]
    if last:
        width = w_value.shape[2]
        operands.append(w_value)
        in_specs.append(by_head(w_value))
        out_shape = jax.ShapeDtypeStruct((tokens, all_heads * width), jnp.bfloat16)
        out_specs = pl.BlockSpec((tokens, heads * width), lambda g: (0, g))
    else:
        out_shape = tuple(
            jax.ShapeDtypeStruct((all_heads, tokens, width), jnp.float32)
            for width in (KV_RANK, LANES, LANES)
        )
        out_specs = tuple(by_head(a) for a in out_shape)
    return pl.pallas_call(
        functools.partial(attend_kernel, tags, first, last),
        out_shape=out_shape,
        grid=(all_heads // heads,),
        in_specs=in_specs,
        out_specs=out_specs,
        input_output_aliases={} if first or last else {len(operands) - len(state) + i: i for i in range(len(state))},
        compiler_params=pltpu.CompilerParams(vmem_limit_bytes=VMEM_LIMIT),
        cost_estimate=pl.CostEstimate(
            flops=2 * all_heads * tokens * count * (2 * KV_RANK + ROPE),
            bytes_accessed=2 * all_heads * tokens * (KV_RANK + ROPE),
            transcendentals=all_heads * tokens * count,
        ),
        name="attend",
    )(*operands)


def shards(seq_size, tp_size, hidden, w_kv_down, kv_gain, q_latent, q_rope, w_value):
    tokens = hidden.shape[0]
    heads = q_latent.shape[1]
    index = lax.axis_index("seq")
    positions = index * tokens + jnp.arange(tokens, dtype=jnp.int32)
    index = index.reshape(1)

    def from_seq(value, xor):
        return lax.ppermute(value, "seq", [(i, i ^ xor) for i in range(seq_size)])

    def from_below(value, planes):
        shift = planes * GROUP
        return lax.ppermute(value, "seq", [(i, i + shift) for i in range(seq_size - shift)])

    own = down_project(hidden, w_kv_down.T)
    stride = 1
    while True:
        other = lax.ppermute(own, "tp", [(i, i ^ stride) for i in range(tp_size)])
        stride *= 2
        if stride >= tp_size:
            break
        own = own + other
    cosine, sine = tables(positions)
    latent = lax.optimization_barrier(jnp.transpose(q_latent, (1, 0, 2)))
    gain = jnp.broadcast_to(kv_gain[:, None], (KV_RANK, tokens))
    rope = rotate(q_rope, *query_tables(positions), heads)
    key_here = finish(own, other, gain, cosine, sine, latent[:1, :16, :LANES], rope)

    levels = range(1, seq_size // GROUP)
    key_y = from_seq(key_here, 2)
    below = {d: from_below(key_here, d) for d in levels if d != 2}
    if 2 in levels:
        below[2] = from_below(below[1], 1)
    below = {d: below[d] for d in levels}
    plane = [key_here, key_y, from_seq(key_here, 1), from_seq(key_y, 1)]
    below_y = {d: from_seq(below[d], 2) for d in levels}
    below_core = {d: from_seq(below[d], 1) for d in levels}
    below_yc = {d: from_seq(below_y[d], 1) for d in levels}
    tag = lambda group: [(("below", d), group[d]) for d in group]

    state = attend(index, latent, rope, [(("plane", x), k) for x, k in zip((0, 2, 1, 3), plane)])
    early = tag(below) + tag({1: below_y[1]})
    late = tag({d: below_y[d] for d in levels if d > 1}) + tag(below_core) + tag(below_yc)
    early, late = (sorted(group, key=lambda item: item[0][1]) for group in (early, late))
    state = attend(index, latent, rope, early, state=state)
    return attend(index, latent, rope, late, state=state, w_value=w_value)


def solution(mesh):
    placed = (
        P("seq", "tp"),
        P("tp", None),
        P(),
        P("seq", "tp", None),
        P("seq", "tp"),
        P("tp", None, None),
    )
    body = functools.partial(shards, mesh.shape["seq"], mesh.shape["tp"])

    return jax.shard_map(
        body, mesh=mesh, in_specs=placed, out_specs=P("seq", "tp"), check_vma=False
    )
```

```python
import functools

import jax
import jax.numpy as jnp
from jax import lax
from jax.experimental import pallas as pl
from jax.experimental.pallas import tpu as pltpu
from jax.sharding import PartitionSpec as P


KV_RANK = 512
ROPE = 64
LANES = 128
GROUP = 4

SCORE_SCALE = 192.0 ** (-0.5)
LOG2_E = 1.4426950408889634
EXP2_SCALE = SCORE_SCALE * LOG2_E
ROPE_BASE = 10000.0
EPSILON = 1e-06
MASKED = -1e30
CHUNK = 4
VMEM_LIMIT = 24 * 1024 * 1024
SMALL_VMEM = 8 * 1024 * 1024
FULL_VMEM = 60 * 1024 * 1024
PROJECT_STEPS = (896, 512, 256, 128)


def tables(positions):
    half = ROPE // 2
    frequency = ROPE_BASE ** (-jnp.arange(half, dtype=jnp.float32) * 2.0 / ROPE)
    angles = frequency[:, None] * positions.astype(jnp.float32)[None, :]
    return jnp.cos(angles), jnp.sin(angles)


def query_tables(positions):
    half = ROPE // 2
    frequency = ROPE_BASE ** (-jnp.arange(half, dtype=jnp.float32) * 2.0 / ROPE)
    angles = positions.astype(jnp.float32)[:, None] * frequency[None, :]
    cosine, sine = jnp.cos(angles), jnp.sin(angles)
    return jnp.concatenate([cosine] * 4, -1), jnp.concatenate([-sine, sine] * 2, -1)


def project_kernel(hidden_ref, weight_ref, out_ref, hidden_vmem, weight_vmem, sems):
    depth = hidden_ref.shape[1]
    steps = sems.shape[1]
    size = depth // steps
    copies = []
    for k in range(steps):
        at = pl.ds(k * size, size)
        pair = (
            pltpu.make_async_copy(weight_ref.at[:, at], weight_vmem.at[:, at], sems.at[0, k]),
            pltpu.make_async_copy(hidden_ref.at[:, at], hidden_vmem.at[:, at], sems.at[1, k]),
        )
        for copy in pair:
            copy.start()
        copies.append(pair)
    total = None
    for k, pair in enumerate(copies):
        for copy in pair:
            copy.wait()
        at = slice(k * size, (k + 1) * size)
        part = lax.dot_general(
            weight_vmem[:, at],
            hidden_vmem[:, at],
            (((1,), (1,)), ((), ())),
            preferred_element_type=jnp.float32,
        )
        total = part if total is None else total + part
    out_ref[...] = total


def down_project(hidden, weight_t):
    rows, depth = hidden.shape
    width = weight_t.shape[0]
    size = next(s for s in PROJECT_STEPS if depth % s == 0)
    return pl.pallas_call(
        project_kernel,
        out_shape=jax.ShapeDtypeStruct((width, rows), jnp.float32),
        in_specs=[pl.BlockSpec(memory_space=pltpu.HBM)] * 2,
        out_specs=pl.BlockSpec(memory_space=pltpu.VMEM),
        scratch_shapes=[
            pltpu.VMEM(hidden.shape, hidden.dtype),
            pltpu.VMEM(weight_t.shape, weight_t.dtype),
            pltpu.SemaphoreType.DMA((2, depth // size)),
        ],
        cost_estimate=pl.CostEstimate(
            flops=2 * rows * depth * width, bytes_accessed=2 * depth * (rows + width), transcendentals=0
        ),
        compiler_params=pltpu.CompilerParams(vmem_limit_bytes=FULL_VMEM),
        name="down_project",
    )(hidden, weight_t)


def finish_kernel(own_ref, other_ref, gain_ref, cos_ref, sin_ref, latent_ref, rope_ref, out_ref):
    del latent_ref, rope_ref
    projection = own_ref[...] + other_ref[...]
    latent = projection[:KV_RANK]
    mean_square = jnp.mean(latent * latent, axis=0, keepdims=True)
    normed = latent * lax.rsqrt(mean_square + EPSILON) * gain_ref[...]
    half = ROPE // 2
    first, second = projection[KV_RANK : KV_RANK + half], projection[KV_RANK + half :]
    cosine, sine = cos_ref[...], sin_ref[...]
    keys = [normed, first * cosine - second * sine, first * sine + second * cosine]
    out_ref[...] = jnp.concatenate(keys, 0).astype(jnp.bfloat16)


def finish(own, other, gain, cosine, sine, latent, rope):
    return pl.pallas_call(
        finish_kernel,
        out_shape=jax.ShapeDtypeStruct(own.shape, jnp.bfloat16),
        in_specs=[pl.BlockSpec(memory_space=pltpu.VMEM)] * 5 + [pl.BlockSpec(memory_space=pl.ANY)] * 2,
        out_specs=pl.BlockSpec(memory_space=pltpu.VMEM),
        compiler_params=pltpu.CompilerParams(vmem_limit_bytes=SMALL_VMEM),
        name="finish_keys",
    )(own, other, gain, cosine, sine, latent, rope)


def rotate_kernel(query_ref, cos_ref, sin_ref, out_ref):
    cosine, sine = cos_ref[...], sin_ref[...]
    half = ROPE // 2
    lower = lax.broadcasted_iota(jnp.int32, cosine.shape, 1) % ROPE < half
    for pair in range(query_ref.shape[1] // (2 * ROPE)):
        value = query_ref[:, pair * 2 * ROPE : (pair + 1) * 2 * ROPE].astype(jnp.float32)
        up, down = pltpu.roll(value, 2 * ROPE - half, 1), pltpu.roll(value, half, 1)
        rotated = value * cosine + jnp.where(lower, up, down) * sine
        out_ref[2 * pair] = rotated[:, :ROPE].astype(jnp.bfloat16)
        out_ref[2 * pair + 1] = rotated[:, ROPE:].astype(jnp.bfloat16)


def rotate(query, cosine, sine, heads):
    return pl.pallas_call(
        rotate_kernel,
        out_shape=jax.ShapeDtypeStruct((heads, query.shape[0], ROPE), jnp.bfloat16),
        compiler_params=pltpu.CompilerParams(vmem_limit_bytes=SMALL_VMEM),
        name="rotate_queries",
    )(query, cosine, sine)


def block_bias(index, tag, tokens, rows):
    kind, amount = tag
    if kind == "plane":
        key = (index ^ amount) * tokens + lax.broadcasted_iota(jnp.int32, (rows, tokens), 1)
        query = index * tokens + lax.broadcasted_iota(jnp.int32, (rows, tokens), 0)
        return jnp.where(key <= query, 0.0, MASKED)
    return jnp.full((rows, tokens), jnp.where(index // GROUP >= amount, 0.0, MASKED), jnp.float32)


def attend_kernel(tags, first, last, index_ref, latent_ref, rope_ref, *refs):
    key_refs, rest = refs[: len(tags)], list(refs[len(tags) :])
    heads, tokens = latent_ref.shape[:2]
    rows = heads * tokens
    index = index_ref[0]
    state_refs = [] if first else rest[:3]
    rest = rest[len(state_refs) :]
    cut = lambda count: [range(b, min(b + CHUNK, count)) for b in range(0, count, CHUNK)]
    wide = lambda column: jnp.broadcast_to(column, (rows, LANES))
    spread = lambda value, width: jnp.concatenate([value] * (width // LANES), -1)

    def run(groups):
        top = total = mixed = None
        if not first:
            mixed, top, total = (ref[...].reshape(rows, ref.shape[2]) for ref in state_refs)
        if groups:
            query = jnp.concatenate(
                [latent_ref[...].reshape(rows, KV_RANK), rope_ref[...].reshape(rows, ROPE)], -1
            )
        for group in groups:
            keys = jnp.concatenate([key_refs[i][...] for i in group], 1)
            count = keys.shape[1]
            scores = jnp.dot(query, keys, preferred_element_type=jnp.float32)
            plane = tags[group[0]][0] == "plane"
            bias = jnp.concatenate(
                [block_bias(index, tags[i], tokens, tokens if plane else 1) for i in group], -1
            )
            if plane:
                scores = (scores.reshape(heads, tokens, count) + bias[None]).reshape(rows, count)
            else:
                scores = scores + bias
            chunk_top = wide(jnp.max(scores, axis=-1, keepdims=True))
            new_top = chunk_top if top is None else jnp.maximum(top, chunk_top)
            weights = jnp.exp2((scores - spread(new_top, count)) * EXP2_SCALE)
            chunk_total = wide(jnp.sum(weights, axis=-1, keepdims=True))
            chunk_mixed = lax.dot_general(
                weights.astype(jnp.bfloat16),
                keys[:KV_RANK],
                (((1,), (1,)), ((), ())),
                preferred_element_type=jnp.float32,
            )
            if top is None:
                total, mixed = chunk_total, chunk_mixed
            else:
                rescale = jnp.exp2((top - new_top) * EXP2_SCALE)
                total = total * rescale + chunk_total
                mixed = mixed * spread(rescale, KV_RANK) + chunk_mixed
            top = new_top
        if last:
            value_ref, out_ref = rest
            latent_out = (mixed / spread(total, KV_RANK)).astype(jnp.bfloat16)
            width = value_ref.shape[2]
            for h in range(heads):
                out_ref[:, h * width : (h + 1) * width] = jnp.dot(
                    latent_out[h * tokens : (h + 1) * tokens],
                    value_ref[h],
                    preferred_element_type=jnp.float32,
                ).astype(jnp.bfloat16)
        else:
            for ref, value in zip(rest, (mixed, top, total)):
                ref[...] = value.reshape(ref.shape)

    if first:
        run(cut(len(tags)))
        return
    levels = sorted({level for _, level in tags})
    bounds = [0] + (levels if len(levels) <= 3 else levels[:2] + levels[-1:])
    plane = index // GROUP
    for below, bound in zip([-1] + bounds, bounds):
        count = sum(level <= bound for _, level in tags)
        inside = plane > below if bound == levels[-1] else (plane > below) & (plane <= bound)

        @pl.when(inside)
        def _():
            run(cut(count))


def attend(index, latent, rope, tagged, state=(), w_value=None):
    first, last = not state, w_value is not None
    tags, keys = zip(*tagged)
    all_heads, tokens, _ = latent.shape
    heads = next(h for h in (8, 4, 2, 1) if all_heads % h == 0)
    count = sum(k.shape[1] for k in keys)
    by_head = lambda a: pl.BlockSpec((heads,) + a.shape[1:], lambda g: (g, 0, 0))
    whole = lambda a: pl.BlockSpec(a.shape, lambda g: (0,) * a.ndim)
    operands = [index, latent, rope, *keys, *state]
    in_specs = [pl.BlockSpec(memory_space=pltpu.SMEM), by_head(latent), by_head(rope)]
    in_specs += [whole(k) for k in keys] + [by_head(a) for a in state]
    if last:
        width = w_value.shape[2]
        operands.append(w_value)
        in_specs.append(by_head(w_value))
        out_shape = jax.ShapeDtypeStruct((tokens, all_heads * width), jnp.bfloat16)
        out_specs = pl.BlockSpec((tokens, heads * width), lambda g: (0, g))
    else:
        out_shape = tuple(
            jax.ShapeDtypeStruct((all_heads, tokens, width), jnp.float32)
            for width in (KV_RANK, LANES, LANES)
        )
        out_specs = tuple(by_head(a) for a in out_shape)
    return pl.pallas_call(
        functools.partial(attend_kernel, tags, first, last),
        out_shape=out_shape,
        grid=(all_heads // heads,),
        in_specs=in_specs,
        out_specs=out_specs,
        input_output_aliases={} if first or last else {len(operands) - len(state) + i: i for i in range(len(state))},
        compiler_params=pltpu.CompilerParams(vmem_limit_bytes=VMEM_LIMIT),
        cost_estimate=pl.CostEstimate(
            flops=2 * all_heads * tokens * count * (2 * KV_RANK + ROPE),
            bytes_accessed=2 * all_heads * tokens * (KV_RANK + ROPE),
            transcendentals=all_heads * tokens * count,
        ),
        name="attend",
    )(*operands)


def shards(seq_size, tp_size, hidden, w_kv_down, kv_gain, q_latent, q_rope, w_value):
    tokens = hidden.shape[0]
    heads = q_latent.shape[1]
    index = lax.axis_index("seq")
    positions = index * tokens + jnp.arange(tokens, dtype=jnp.int32)
    index = index.reshape(1)

    def from_seq(value, xor):
        return lax.ppermute(value, "seq", [(i, i ^ xor) for i in range(seq_size)])

    def from_below(value, planes):
        shift = planes * GROUP
        return lax.ppermute(value, "seq", [(i, i + shift) for i in range(seq_size - shift)])

    own = down_project(hidden, w_kv_down.T)
    stride = 1
    while True:
        other = lax.ppermute(own, "tp", [(i, i ^ stride) for i in range(tp_size)])
        stride *= 2
        if stride >= tp_size:
            break
        own = own + other
    cosine, sine = tables(positions)
    latent = lax.optimization_barrier(jnp.transpose(q_latent, (1, 0, 2)))
    gain = jnp.broadcast_to(kv_gain[:, None], (KV_RANK, tokens))
    rope = rotate(q_rope, *query_tables(positions), heads)
    key_here = finish(own, other, gain, cosine, sine, latent[:1, :16, :LANES], rope)

    levels = range(1, seq_size // GROUP)
    key_y = from_seq(key_here, 2)
    below = {d: from_below(key_here, d) for d in levels if d != 2}
    if 2 in levels:
        below[2] = from_below(below[1], 1)
    below = {d: below[d] for d in levels}
    plane = [key_here, key_y, from_seq(key_here, 1), from_seq(key_y, 1)]
    below_y = {d: from_seq(below[d], 2) for d in levels}
    below_core = {d: from_seq(below[d], 1) for d in levels}
    below_yc = {d: from_seq(below_y[d], 1) for d in levels}
    tag = lambda group: [(("below", d), group[d]) for d in group]

    state = attend(index, latent, rope, [(("plane", x), k) for x, k in zip((0, 2, 1, 3), plane)])
    early = tag(below) + tag({1: below_y[1]})
    late = tag({d: below_y[d] for d in levels if d > 1}) + tag(below_core) + tag(below_yc)
    early, late = (sorted(group, key=lambda item: item[0][1]) for group in (early, late))
    state = attend(index, latent, rope, early, state=state)
    return attend(index, latent, rope, late, state=state, w_value=w_value)


def solution(mesh):
    placed = (
        P("seq", "tp"),
        P("tp", None),
        P(),
        P("seq", "tp", None),
        P("seq", "tp"),
        P("tp", None, None),
    )
    body = functools.partial(shards, mesh.shape["seq"], mesh.shape["tp"])

    return jax.shard_map(
        body, mesh=mesh, in_specs=placed, out_specs=P("seq", "tp"), check_vma=False
    )
```
